128 devices in a mesh: dap: 2 (over core), dp: 64 (over z, y, x).
Axes of the slice: x: 4, y: 4, z: 4, core: 2. Of those that a mesh axis runs over, the one named last changes fastest.
Arguments:
- pair_z: bfloat16 [192, 96, 96, 128], P('dp', 'dap')
- single_s: bfloat16 [192, 96, 384], P('dp', 'dap')
- token_mask: int32 [192, 96], P('dp')
- dz_out: bfloat16 [192, 96, 96, 128], P('dp', 'dap')
- ds_out: bfloat16 [192, 96, 384], P('dp', 'dap')
- w_pa: bfloat16 [128, 512], replicated
- w_pb: bfloat16 [128, 512], replicated
- w_po: bfloat16 [512, 128], replicated
- w_bias: bfloat16 [128, 16], replicated
- w_q: bfloat16 [384, 384], replicated
- q_bias: bfloat16 [384], replicated
- w_kv: bfloat16 [384, 768], replicated
- w_g: bfloat16 [384, 384], replicated
- w_o: bfloat16 [384, 384], replicated
- w_sa: bfloat16 [384, 1536], replicated
- w_sb: bfloat16 [384, 1536], replicated
- w_so: bfloat16 [1536, 384], replicated
Outputs:
- output 1: bfloat16 [192, 96, 96, 128], P('dp', 'dap')
- output 2: bfloat16 [192, 96, 384], P('dp', 'dap')
- output 3: float32 [128, 512], replicated
- output 4: float32 [128, 512], replicated
- output 5: float32 [512, 128], replicated
- output 6: float32 [128, 16], replicated
- output 7: float32 [384, 384], replicated
- output 8: float32 [384], replicated
- output 9: float32 [384, 768], replicated
- output 10: float32 [384, 384], replicated
- output 11: float32 [384, 384], replicated
- output 12: float32 [384, 1536], replicated
- output 13: float32 [384, 1536], replicated
- output 14: float32 [1536, 384], replicated
All inputs are finite; a program needn't handle non-finite values.
Results may differ from the reference program's by a relative error of at most 0.0184928.
Values are sent between devices in bfloat16 or wider.
A program may use at most 1 GiB of HBM per device.

```python
import jax
import jax.numpy as jnp
from jax import lax

C_S = 384
C_Z = 128
HEADS = 16
HEAD = 24
TRANS = 4
TOKENS = 96
COMPLEXES = 192


def snap_bf16(values):
    return values + lax.stop_gradient(values.astype(jnp.bfloat16).astype(jnp.float32) - values)


def layer_norm(values):
    centred = values - jnp.mean(values, axis=-1, keepdims=True)
    return centred * lax.rsqrt(jnp.mean(centred * centred, axis=-1, keepdims=True) + 1e-5)


def pair_rows(z_rows, w_pa, w_pb, w_po):
    normed = snap_bf16(layer_norm(z_rows))
    hid_a = jnp.einsum('rjc,cf->rjf', normed, w_pa)
    hid_b = jnp.einsum('rjc,cf->rjf', normed, w_pb)
    hidden = snap_bf16(jax.nn.silu(hid_a) * hid_b)
    return snap_bf16(z_rows + jnp.einsum('rjf,fc->rjc', hidden, w_po))


def block_forward(pair_z, single_s, mask_row, w_pa, w_pb, w_po, w_bias, w_q, q_bias, w_kv, w_g, w_o, w_sa, w_sb, w_so):
    attn_width = HEADS * HEAD
    checked_rows = jax.checkpoint(pair_rows)

    def row_step(z_rows):
        return checked_rows(z_rows, w_pa, w_pb, w_po)

    z_new = lax.map(row_step, pair_z.reshape(TOKENS // 16, 16, TOKENS, C_Z)).reshape(TOKENS, TOKENS, C_Z)
    pair_bias = jnp.einsum('ijc,ch->hij', snap_bf16(layer_norm(z_new)), w_bias)
    act_norm = snap_bf16(layer_norm(single_s))
    queries = snap_bf16(jnp.dot(act_norm, w_q, preferred_element_type=jnp.float32) + q_bias).reshape(TOKENS, HEADS, HEAD)
    key_val = snap_bf16(jnp.dot(act_norm, w_kv, preferred_element_type=jnp.float32))
    key_heads = key_val[:, :attn_width].reshape(TOKENS, HEADS, HEAD)
    value_heads = key_val[:, attn_width:].reshape(TOKENS, HEADS, HEAD)
    gate_vals = jax.nn.sigmoid(jnp.dot(act_norm, w_g, preferred_element_type=jnp.float32))
    key_mask = 1e9 * (mask_row.astype(jnp.float32) - 1.0)
    logits = jnp.einsum('ihd,jhd->hij', queries, key_heads) * (HEAD ** -0.5) + pair_bias + key_mask[None, None, :]
    attn_prob = snap_bf16(jax.nn.softmax(logits, axis=-1))
    attended = jnp.einsum('hij,jhd->ihd', attn_prob, value_heads).reshape(TOKENS, attn_width)
    gated = snap_bf16(gate_vals * attended)
    s_mid = snap_bf16(single_s + jnp.dot(gated, w_o, preferred_element_type=jnp.float32))
    mid_act = snap_bf16(layer_norm(s_mid))
    trans_a = jnp.dot(mid_act, w_sa, preferred_element_type=jnp.float32)
    trans_b = jnp.dot(mid_act, w_sb, preferred_element_type=jnp.float32)
    trans_hidden = snap_bf16(jax.nn.silu(trans_a) * trans_b)
    return z_new, s_mid + jnp.dot(trans_hidden, w_so, preferred_element_type=jnp.float32)


def draw_mask(mask_key):
    len_key, full_key = jax.random.split(mask_key)
    lengths = jax.random.randint(len_key, (COMPLEXES,), TOKENS // 4, TOKENS + 1)
    full_at = jax.random.randint(full_key, (), 0, COMPLEXES)
    lengths = jnp.where(jnp.arange(COMPLEXES) == full_at, TOKENS, lengths)
    return (jnp.arange(TOKENS)[None, :] < lengths[:, None]).astype(jnp.int32)


def setup_inputs(seed: int = 0) -> dict:
    sub_keys = jax.random.split(jax.random.key(seed), 17)
    attn_width = HEADS * HEAD

    def draw_normal(key_index, arr_shape, std_scale):
        return (jax.random.normal(sub_keys[key_index], arr_shape, jnp.float32) * std_scale).astype(jnp.bfloat16)

    return {
        'pair_z': draw_normal(0, (COMPLEXES, TOKENS, TOKENS, C_Z), 1.0),
        'single_s': draw_normal(1, (COMPLEXES, TOKENS, C_S), 1.0),
        'token_mask': draw_mask(sub_keys[2]),
        'dz_out': draw_normal(3, (COMPLEXES, TOKENS, TOKENS, C_Z), 1.0),
        'ds_out': draw_normal(4, (COMPLEXES, TOKENS, C_S), 1.0),
        'w_pa': draw_normal(5, (C_Z, TRANS * C_Z), C_Z ** -0.5),
        'w_pb': draw_normal(6, (C_Z, TRANS * C_Z), C_Z ** -0.5),
        'w_po': draw_normal(7, (TRANS * C_Z, C_Z), (TRANS * C_Z) ** -0.5),
        'w_bias': draw_normal(8, (C_Z, HEADS), C_Z ** -0.5),
        'w_q': draw_normal(9, (C_S, attn_width), C_S ** -0.5),
        'q_bias': draw_normal(10, (attn_width,), 0.5),
        'w_kv': draw_normal(11, (C_S, 2 * attn_width), C_S ** -0.5),
        'w_g': draw_normal(12, (C_S, attn_width), C_S ** -0.5),
        'w_o': draw_normal(13, (attn_width, C_S), attn_width ** -0.5),
        'w_sa': draw_normal(14, (C_S, TRANS * C_S), C_S ** -0.5),
        'w_sb': draw_normal(15, (C_S, TRANS * C_S), C_S ** -0.5),
        'w_so': draw_normal(16, (TRANS * C_S, C_S), (TRANS * C_S) ** -0.5),
    }


def reference(pair_z, single_s, token_mask, dz_out, ds_out, w_pa, w_pb, w_po, w_bias, w_q, q_bias, w_kv, w_g, w_o, w_sa, w_sb, w_so):
    weights = tuple(weight.astype(jnp.float32) for weight in (w_pa, w_pb, w_po, w_bias, w_q, q_bias, w_kv, w_g, w_o, w_sa, w_sb, w_so))

    def scan_step(running, per_complex):
        z_one, s_one, mask_one, dz_one, ds_one = per_complex

        def run_block(z_in, s_in, *params):
            return block_forward(z_in, s_in, mask_one, *params)

        _, pullback = jax.vjp(run_block, z_one.astype(jnp.float32), s_one.astype(jnp.float32), *weights)
        all_grads = pullback((dz_one.astype(jnp.float32), ds_one.astype(jnp.float32)))
        summed = tuple(acc_sum + update for acc_sum, update in zip(running, all_grads[2:]))
        return summed, (all_grads[0].astype(jnp.bfloat16), all_grads[1].astype(jnp.bfloat16))

    zero_sums = tuple(jnp.zeros_like(weight) for weight in weights)
    grad_sums, (dz_in, ds_in) = lax.scan(scan_step, zero_sums, (pair_z, single_s, token_mask, dz_out, ds_out))
    return (dz_in, ds_in, grad_sums[0], grad_sums[1], grad_sums[2], grad_sums[3], grad_sums[4], grad_sums[5], grad_sums[6], grad_sums[7], grad_sums[8], grad_sums[9], grad_sums[10], grad_sums[11])
```

```python
import functools
import jax
import jax.numpy as jnp
from jax import lax
from jax.experimental import pallas as pl
from jax.experimental.pallas import tpu as pltpu
from jax.sharding import PartitionSpec as P

HEADS = 16
HEAD_DIM = 24
EPSILON = 1e-5
MASK_BIG = 1e9
SCALE = HEAD_DIM ** -0.5
ROWS = 8
F32 = jnp.float32
BF16 = jnp.bfloat16

Q_AT, G_AT, O_AT, K_AT, V_AT, SO_AT, SA_AT, SB_AT, QB_AT, PACK_ROWS = 0, 384, 768, 1152, 1536, 1920, 3456, 4992, 6528, 6656


def dot(left, right):
    return lax.dot_general(left, right, (((1,), (0,)), ((), ())), preferred_element_type=F32)


def dot_rt(left, right):
    return lax.dot_general(left, right, (((1,), (1,)), ((), ())), preferred_element_type=F32)


def dot_lt(left, right):
    return lax.dot_general(left, right, (((0,), (0,)), ((), ())), preferred_element_type=F32)


def layer_norm(values):
    wide = values.astype(F32)
    centred = wide - jnp.mean(wide, axis=-1, keepdims=True)
    inv_std = lax.rsqrt(jnp.mean(centred * centred, axis=-1, keepdims=True) + EPSILON)
    return centred * inv_std, inv_std


def norm_grad(normed, inv_std, grad_out):
    mean_grad = jnp.mean(grad_out, axis=-1, keepdims=True)
    mean_proj = jnp.mean(grad_out * normed, axis=-1, keepdims=True)
    return inv_std * (grad_out - mean_grad - normed * mean_proj)


def sigmoid(values):
    return jax.nn.sigmoid(values)


def pair_forward_kernel(z_ref, wpab_ref, wpo_ref, wbt_ref, znew_ref, bias_ref):
    step = pl.program_id(1)
    num_tok = z_ref.shape[2]
    num_rows = bias_ref.shape[1] // HEADS
    z_rows = z_ref[0].reshape(ROWS * num_tok, z_ref.shape[3])
    normed, _ = layer_norm(z_rows)
    hid = dot(normed.astype(BF16), wpab_ref[...])
    width = wpo_ref.shape[0]
    hid_a, hid_b = hid[:, :width], hid[:, width:]
    hidden = (hid_a * sigmoid(hid_a) * hid_b).astype(BF16)
    z_new = (z_rows.astype(F32) + dot(hidden, wpo_ref[...])).astype(BF16)
    znew_ref[0] = z_new.reshape(ROWS, num_tok, z_new.shape[1])
    bias_norm, _ = layer_norm(z_new)
    bias_bf = bias_norm.astype(BF16)
    for r in range(ROWS):
        bias_ref[0, pl.ds(step * ROWS + r, HEADS, stride=num_rows), :] = dot_rt(wbt_ref[...], bias_bf[r * num_tok:(r + 1) * num_tok])


def pair_backward_kernel(z_ref, znew_ref, dz_ref, dl_ref, wpab_ref, wpo_ref, wbt_ref, dzin_ref, dwab_ref, dwot_ref, dwbt_ref):
    step = pl.program_id(1)
    num_tok, chans = z_ref.shape[2], z_ref.shape[3]
    num_rows = dl_ref.shape[1] // HEADS
    width = wpo_ref.shape[0]
    flat = (ROWS * num_tok, chans)

    @pl.when(jnp.logical_and(pl.program_id(0) == 0, step == 0))
    def _():
        dwab_ref[...] = jnp.zeros_like(dwab_ref)
        dwot_ref[...] = jnp.zeros_like(dwot_ref)
        dwbt_ref[...] = jnp.zeros_like(dwbt_ref)

    bias_norm, bias_inv = layer_norm(znew_ref[0].reshape(flat))
    bias_bf = bias_norm.astype(BF16)
    grad_rows = []
    d_bias_t = jnp.zeros(dwbt_ref.shape, F32)
    for r in range(ROWS):
        dl_row = dl_ref[0, pl.ds(step * ROWS + r, HEADS, stride=num_rows), :].astype(BF16)
        grad_rows.append(dot_lt(dl_row, wbt_ref[...]))
        d_bias_t += dot(dl_row, bias_bf[r * num_tok:(r + 1) * num_tok])
    dwbt_ref[...] += d_bias_t
    grad_norm = jnp.concatenate(grad_rows, axis=0)
    grad_new = dz_ref[0].reshape(flat).astype(F32) + norm_grad(bias_norm, bias_inv, grad_norm)
    grad_new_bf = grad_new.astype(BF16)
    normed, inv_std = layer_norm(z_ref[0].reshape(flat))
    normed_bf = normed.astype(BF16)
    hid = dot(normed_bf, wpab_ref[...])
    grad_hidden = dot_rt(grad_new_bf, wpo_ref[...])
    hid_a, hid_b = hid[:, :width], hid[:, width:]
    sig_a = sigmoid(hid_a)
    silu_a = hid_a * sig_a
    hidden = (silu_a * hid_b).astype(BF16)
    grad_b = (grad_hidden * silu_a).astype(BF16)
    grad_a = (grad_hidden * hid_b * (sig_a + silu_a * (1.0 - sig_a))).astype(BF16)
    dwot_ref[...] += dot_lt(grad_new_bf, hidden)
    dwab_ref[:, :width] += dot_lt(normed_bf, grad_a)
    dwab_ref[:, width:] += dot_lt(normed_bf, grad_b)
    grad_normed = dot_rt(grad_a, wpab_ref[:, :width]) + dot_rt(grad_b, wpab_ref[:, width:])
    dz_in = grad_new + norm_grad(normed, inv_std, grad_normed)
    dzin_ref[0] = dz_in.astype(BF16).reshape(ROWS, num_tok, chans)


def single_kernel(idx_ref, own_ref, other_ref, mask_ref, ds_ref, bias_ref, wq_ref, qb_ref, wkv_ref, wg_ref, wo_ref, wsa_ref, wsb_ref, wso_ref,
                  pack_ref, dl_ref, send_ref, mid_ref, act_ref, full_scr, part_scr):
    idx = idx_ref[0]
    num_cplx, num_rows, chans = own_ref.shape
    num_tok = 2 * num_rows
    for c in range(num_cplx):
        full_scr[pl.ds(pl.multiple_of(c * num_tok + idx * num_rows, 16), num_rows), :] = own_ref[c]
        full_scr[pl.ds(pl.multiple_of(c * num_tok + (1 - idx) * num_rows, 16), num_rows), :] = other_ref[c]
    s_own = own_ref[...].reshape(num_cplx * num_rows, chans)
    s_norm, s_inv = layer_norm(s_own)
    act = s_norm.astype(BF16)
    act_all = layer_norm(full_scr[...])[0].astype(BF16)
    queries = (dot(act, wq_ref[...]) + qb_ref[...].astype(F32)).astype(BF16)
    key_val = dot(act_all, wkv_ref[...]).astype(BF16)
    gate = sigmoid(dot(act, wg_ref[...]))
    lane = lax.broadcasted_iota(jnp.int32, (1, chans), 1)
    head_masks = [jnp.where((lane >= h * HEAD_DIM) & (lane < (h + 1) * HEAD_DIM), 1.0, 0.0) for h in range(HEADS)]

    def spread(values):
        return jnp.concatenate([values * head_masks[h].astype(BF16) for h in range(HEADS)], axis=0)

    def gather_heads(stacked):
        total = stacked[:num_rows] * head_masks[0]
        for h in range(1, HEADS):
            total += stacked[h * num_rows:(h + 1) * num_rows] * head_masks[h]
        return total

    probs, att_rows = [], []
    for c in range(num_cplx):
        keys = key_val[c * num_tok:(c + 1) * num_tok, :chans]
        values = key_val[c * num_tok:(c + 1) * num_tok, chans:]
        key_mask = MASK_BIG * (mask_ref[c:c + 1, :].astype(F32) - 1.0)
        logits = dot_rt(spread(queries[c * num_rows:(c + 1) * num_rows]), keys) * SCALE + bias_ref[c] + key_mask
        expo = jnp.exp(logits - jnp.max(logits, axis=-1, keepdims=True))
        prob = expo / jnp.sum(expo, axis=-1, keepdims=True)
        probs.append(prob)
        att_rows.append(gather_heads(dot(prob.astype(BF16), values)))
    attended = jnp.concatenate(att_rows, axis=0)
    gated = (gate * attended).astype(BF16)
    s_mid = (s_own.astype(F32) + dot(gated, wo_ref[...])).astype(BF16)
    mid_norm, mid_inv = layer_norm(s_mid)
    mid_act = mid_norm.astype(BF16)
    trans_a = dot(mid_act, wsa_ref[...])
    trans_b = dot(mid_act, wsb_ref[...])
    sig_a = sigmoid(trans_a)
    silu_a = trans_a * sig_a
    hidden = (silu_a * trans_b).astype(BF16)
    ds_rows = ds_ref[...].reshape(num_cplx * num_rows, chans)
    pack_ref[SO_AT:SA_AT, :] = dot_lt(hidden, ds_rows).astype(BF16)
    grad_hidden = dot_rt(ds_rows, wso_ref[...])
    grad_b = (grad_hidden * silu_a).astype(BF16)
    grad_a = (grad_hidden * trans_b * (sig_a + silu_a * (1.0 - sig_a))).astype(BF16)
    for part in range(4):
        cols = slice(part * chans, (part + 1) * chans)
        pack_ref[SA_AT + part * chans:SA_AT + (part + 1) * chans, :] = dot_lt(mid_act, grad_a[:, cols]).astype(BF16)
        pack_ref[SB_AT + part * chans:SB_AT + (part + 1) * chans, :] = dot_lt(mid_act, grad_b[:, cols]).astype(BF16)
    grad_mid_norm = dot_rt(grad_a, wsa_ref[...]) + dot_rt(grad_b, wsb_ref[...])
    grad_mid = ds_rows.astype(F32) + norm_grad(mid_norm, mid_inv, grad_mid_norm)
    mid_ref[...] = grad_mid
    grad_mid_bf = grad_mid.astype(BF16)
    pack_ref[O_AT:K_AT, :] = dot_lt(gated, grad_mid_bf).astype(BF16)
    grad_gated = dot_rt(grad_mid_bf, wo_ref[...])
    grad_gate = (grad_gated * attended * gate * (1.0 - gate)).astype(BF16)
    grad_att = (grad_gated * gate).astype(BF16)
    query_rows, key_rows, value_rows = [], [], []
    for c in range(num_cplx):
        keys = key_val[c * num_tok:(c + 1) * num_tok, :chans]
        values = key_val[c * num_tok:(c + 1) * num_tok, chans:]
        prob = probs[c]
        att_spread = spread(grad_att[c * num_rows:(c + 1) * num_rows])
        grad_prob = dot_rt(att_spread, values)
        value_rows.append(dot_lt(prob.astype(BF16), att_spread))
        grad_logits = prob * (grad_prob - jnp.sum(prob * grad_prob, axis=-1, keepdims=True))
        grad_bf = grad_logits.astype(BF16)
        dl_ref[c] = grad_bf.astype(F32)
        query_rows.append(gather_heads(dot(grad_bf, keys)) * SCALE)
        key_rows.append(dot_lt(grad_bf, spread(queries[c * num_rows:(c + 1) * num_rows])) * SCALE)
    grad_query = jnp.concatenate(query_rows, axis=0)
    grad_query_bf = grad_query.astype(BF16)
    grad_key_bf = jnp.concatenate(key_rows, axis=0).astype(BF16)
    grad_value_bf = jnp.concatenate(value_rows, axis=0).astype(BF16)
    pack_ref[Q_AT:G_AT, :] = dot_lt(act, grad_query_bf).astype(BF16)
    pack_ref[G_AT:O_AT, :] = dot_lt(act, grad_gate).astype(BF16)
    pack_ref[K_AT:V_AT, :] = dot_lt(act_all, grad_key_bf).astype(BF16)
    pack_ref[V_AT:SO_AT, :] = dot_lt(act_all, grad_value_bf).astype(BF16)
    row = lax.broadcasted_iota(jnp.int32, (PACK_ROWS - QB_AT, 1), 0)
    pack_ref[QB_AT:, :] = jnp.where(row == 0, jnp.sum(grad_query, axis=0, keepdims=True), 0.0).astype(BF16)
    part_scr[...] = dot_rt(grad_key_bf, wkv_ref[:, :chans]) + dot_rt(grad_value_bf, wkv_ref[:, chans:])
    local = dot_rt(grad_query_bf, wq_ref[...]) + dot_rt(grad_gate, wg_ref[...])
    for c in range(num_cplx):
        rows = slice(c * num_rows, (c + 1) * num_rows)
        act_ref[rows, :] = local[rows] + part_scr[pl.ds(pl.multiple_of(c * num_tok + idx * num_rows, 8), num_rows), :]
        send_ref[rows, :] = part_scr[pl.ds(pl.multiple_of(c * num_tok + (1 - idx) * num_rows, 8), num_rows), :].astype(BF16)


def finish_kernel(own_ref, mid_ref, act_ref, recv_ref, out_ref):
    s_norm, s_inv = layer_norm(own_ref[...])
    grad_act = act_ref[...] + recv_ref[...].astype(F32)
    out_ref[...] = (mid_ref[...] + norm_grad(s_norm, s_inv, grad_act)).astype(BF16)


VMEM_LIMIT = 60 * 1024 * 1024


def solution(mesh):
    pair_spec = P('dp', 'dap', None, None)
    single_spec = P('dp', 'dap', None)

    def body(pair_z, single_s, token_mask, dz_out, ds_out, w_pa, w_pb, w_po, w_bias, w_q, q_bias, w_kv, w_g, w_o, w_sa, w_sb, w_so):
        num_cplx, num_rows, num_tok, chans = pair_z.shape
        s_chans = single_s.shape[2]
        width = w_pa.shape[1]
        idx = lax.axis_index('dap')
        swap = [(0, 1), (1, 0)]
        other_s = lax.ppermute(single_s, 'dap', swap)
        w_pab = jnp.concatenate([w_pa, w_pb], axis=1)
        w_bias_t = w_bias.T
        steps = num_rows // ROWS
        row_spec = pl.BlockSpec((1, ROWS, num_tok, chans), lambda c, r: (c, r, 0, 0))
        head_spec = pl.BlockSpec((1, HEADS * num_rows, num_tok), lambda c, r: (c, 0, 0))

        def whole(shape):
            return pl.BlockSpec(shape, lambda c, r: (0,) * len(shape))

        positions = num_cplx * num_rows * num_tok
        z_new, bias = pl.pallas_call(
            pair_forward_kernel,
            grid=(num_cplx, steps),
            in_specs=[row_spec, whole(w_pab.shape), whole(w_po.shape), whole(w_bias_t.shape)],
            out_specs=[row_spec, head_spec],
            out_shape=[jax.ShapeDtypeStruct(pair_z.shape, BF16), jax.ShapeDtypeStruct((num_cplx, HEADS * num_rows, num_tok), F32)],
            compiler_params=pltpu.CompilerParams(dimension_semantics=('arbitrary', 'arbitrary'), vmem_limit_bytes=VMEM_LIMIT),
            cost_estimate=pl.CostEstimate(flops=positions * 3 * 2 * chans * width, bytes_accessed=positions * chans * 4, transcendentals=positions * width),
            name='pair_forward',
        )(pair_z, w_pab, w_po, w_bias_t)

        tokens = num_cplx * num_rows
        pack, d_logits, send, grad_mid, grad_act = pl.pallas_call(
            single_kernel,
            in_specs=[pl.BlockSpec(memory_space=pltpu.SMEM)] + [pl.BlockSpec(memory_space=pltpu.VMEM)] * 13,
            out_specs=[pl.BlockSpec(memory_space=pltpu.VMEM)] * 5,
            out_shape=[
                jax.ShapeDtypeStruct((PACK_ROWS, s_chans), BF16),
                jax.ShapeDtypeStruct((num_cplx, HEADS * num_rows, num_tok), F32),
                jax.ShapeDtypeStruct((tokens, s_chans), BF16),
                jax.ShapeDtypeStruct((tokens, s_chans), F32),
                jax.ShapeDtypeStruct((tokens, s_chans), F32),
            ],
            scratch_shapes=[pltpu.VMEM((2 * tokens, s_chans), BF16), pltpu.VMEM((2 * tokens, s_chans), F32)],
            compiler_params=pltpu.CompilerParams(vmem_limit_bytes=VMEM_LIMIT),
            cost_estimate=pl.CostEstimate(flops=10 ** 10, bytes_accessed=10 ** 7, transcendentals=10 ** 6),
            name='single_path',
        )(idx.reshape(1).astype(jnp.int32), single_s, other_s, token_mask, ds_out, bias, w_q, q_bias.reshape(1, s_chans), w_kv, w_g, w_o, w_sa, w_sb, w_so)

        recv = lax.ppermute(send, 'dap', swap)

        dz_in, d_ab, d_wot, d_wbt = pl.pallas_call(
            pair_backward_kernel,
            grid=(num_cplx, steps),
            in_specs=[row_spec, row_spec, row_spec, head_spec, whole(w_pab.shape), whole(w_po.shape), whole(w_bias_t.shape)],
            out_specs=[row_spec, whole(w_pab.shape), whole((chans, width)), whole(w_bias_t.shape)],
            out_shape=[
                jax.ShapeDtypeStruct(pair_z.shape, BF16),
                jax.ShapeDtypeStruct(w_pab.shape, F32),
                jax.ShapeDtypeStruct((chans, width), F32),
                jax.ShapeDtypeStruct(w_bias_t.shape, F32),
            ],
            compiler_params=pltpu.CompilerParams(dimension_semantics=('arbitrary', 'arbitrary'), vmem_limit_bytes=VMEM_LIMIT),
            cost_estimate=pl.CostEstimate(flops=positions * 8 * 2 * chans * width, bytes_accessed=positions * chans * 8, transcendentals=positions * width),
            name='pair_backward',
        )(pair_z, z_new, dz_out, d_logits, w_pab, w_po, w_bias_t)

        ds_in = pl.pallas_call(
            finish_kernel,
            in_specs=[pl.BlockSpec(memory_space=pltpu.VMEM)] * 4,
            out_specs=pl.BlockSpec(memory_space=pltpu.VMEM),
            out_shape=jax.ShapeDtypeStruct((tokens, s_chans), BF16),
            name='single_finish',
        )(single_s.reshape(tokens, s_chans), grad_mid, grad_act, recv).reshape(single_s.shape)

        pack = lax.psum(pack, ('dap', 'dp')).astype(F32)
        pair_pack = lax.psum(jnp.concatenate([d_ab[:, :width], d_ab[:, width:], d_wot, jnp.pad(d_wbt, ((0, 0), (0, width - chans)))], axis=0).astype(BF16), ('dap', 'dp')).astype(F32)

        def stacked(start, parts):
            return jnp.concatenate([pack[start + p * s_chans:start + (p + 1) * s_chans] for p in range(parts)], axis=1)

        return (dz_in, ds_in, pair_pack[:chans], pair_pack[chans:2 * chans], pair_pack[2 * chans:3 * chans].T,
                pair_pack[3 * chans:3 * chans + HEADS, :chans].T, pack[Q_AT:G_AT], pack[QB_AT], stacked(K_AT, 2),
                pack[G_AT:O_AT], pack[O_AT:K_AT], stacked(SA_AT, 4), stacked(SB_AT, 4), pack[SO_AT:SA_AT])

    in_specs = (pair_spec, single_spec, P('dp', None), pair_spec, single_spec) + (P(),) * 12
    out_specs = (pair_spec, single_spec) + (P(),) * 12
    return jax.shard_map(body, mesh=mesh, in_specs=in_specs, out_specs=out_specs, check_vma=False)
```

```python
import functools
import jax
import jax.numpy as jnp
from jax import lax
from jax.experimental import pallas as pl
from jax.experimental.pallas import tpu as pltpu
from jax.sharding import PartitionSpec as P

HEADS = 16
HEAD_DIM = 24
EPSILON = 1e-5
MASK_BIG = 1e9
SCALE = HEAD_DIM ** -0.5
ROWS = 8
LANES = 128
PAIR_ROWS = 640
MESH = pl.DeviceIdType.MESH
F32 = jnp.float32
BF16 = jnp.bfloat16

Q_AT, G_AT, O_AT, K_AT, V_AT, SO_AT, SA_AT, SB_AT, QB_AT, PACK_ROWS = 0, 384, 768, 1152, 1536, 1920, 3456, 4992, 6528, 6656


def dot(left, right):
    return lax.dot_general(left, right, (((1,), (0,)), ((), ())), preferred_element_type=F32)


def dot_rt(left, right):
    return lax.dot_general(left, right, (((1,), (1,)), ((), ())), preferred_element_type=F32)


def dot_lt(left, right):
    return lax.dot_general(left, right, (((0,), (0,)), ((), ())), preferred_element_type=F32)


def layer_norm(values):
    wide = values.astype(F32)
    centred = wide - jnp.mean(wide, axis=-1, keepdims=True)
    inv_std = lax.rsqrt(jnp.mean(centred * centred, axis=-1, keepdims=True) + EPSILON)
    return centred * inv_std, inv_std


def norm_grad(normed, inv_std, grad_out):
    mean_grad = jnp.mean(grad_out, axis=-1, keepdims=True)
    mean_proj = jnp.mean(grad_out * normed, axis=-1, keepdims=True)
    return inv_std * (grad_out - mean_grad - normed * mean_proj)


def sigmoid(values):
    return jax.nn.sigmoid(values)


def pair_forward_kernel(z_ref, wpa_ref, wpb_ref, wpo_ref, wbt_ref, znew_ref, bias_ref):
    step = pl.program_id(1)
    num_tok = z_ref.shape[2]
    num_rows = bias_ref.shape[1] // HEADS
    z_rows = z_ref[0].reshape(ROWS * num_tok, z_ref.shape[3])
    normed, _ = layer_norm(z_rows)
    normed_bf = normed.astype(BF16)
    hid_a, hid_b = dot(normed_bf, wpa_ref[...]), dot(normed_bf, wpb_ref[...])
    hidden = (hid_a * sigmoid(hid_a) * hid_b).astype(BF16)
    z_new = (z_rows.astype(F32) + dot(hidden, wpo_ref[...])).astype(BF16)
    znew_ref[0] = z_new.reshape(ROWS, num_tok, z_new.shape[1])
    bias_norm, _ = layer_norm(z_new)
    bias_bf = bias_norm.astype(BF16)
    for r in range(ROWS):
        bias_ref[0, pl.ds(step * ROWS + r, HEADS, stride=num_rows), :] = dot_rt(wbt_ref[...], bias_bf[r * num_tok:(r + 1) * num_tok])


def pair_backward_kernel(z_ref, znew_ref, dz_ref, dl_ref, wpa_ref, wpb_ref, wpo_ref, wbt_ref, dzin_ref, pack_ref, dwab_ref, dwot_ref, dwbt_ref):
    step = pl.program_id(1)
    num_tok, chans = z_ref.shape[2], z_ref.shape[3]
    num_rows = dl_ref.shape[1] // HEADS
    width = wpo_ref.shape[0]
    flat = (ROWS * num_tok, chans)

    @pl.when(jnp.logical_and(pl.program_id(0) == 0, step == 0))
    def _():
        dwab_ref[...] = jnp.zeros_like(dwab_ref)
        dwot_ref[...] = jnp.zeros_like(dwot_ref)
        dwbt_ref[...] = jnp.zeros_like(dwbt_ref)

    bias_norm, bias_inv = layer_norm(znew_ref[0].reshape(flat))
    bias_bf = bias_norm.astype(BF16)
    grad_rows = []
    d_bias_t = jnp.zeros(dwbt_ref.shape, F32)
    for r in range(ROWS):
        dl_row = dl_ref[0, pl.ds(step * ROWS + r, HEADS, stride=num_rows), :].astype(BF16)
        grad_rows.append(dot_lt(dl_row, wbt_ref[...]))
        d_bias_t += dot(dl_row, bias_bf[r * num_tok:(r + 1) * num_tok])
    dwbt_ref[...] += d_bias_t
    grad_norm = jnp.concatenate(grad_rows, axis=0)
    grad_new = dz_ref[0].reshape(flat).astype(F32) + norm_grad(bias_norm, bias_inv, grad_norm)
    grad_new_bf = grad_new.astype(BF16)
    normed, inv_std = layer_norm(z_ref[0].reshape(flat))
    normed_bf = normed.astype(BF16)
    hid_a, hid_b = dot(normed_bf, wpa_ref[...]), dot(normed_bf, wpb_ref[...])
    grad_hidden = dot_rt(grad_new_bf, wpo_ref[...])
    sig_a = sigmoid(hid_a)
    silu_a = hid_a * sig_a
    hidden = (silu_a * hid_b).astype(BF16)
    grad_b = (grad_hidden * silu_a).astype(BF16)
    grad_a = (grad_hidden * hid_b * (sig_a + silu_a * (1.0 - sig_a))).astype(BF16)
    dwot_ref[...] += dot_lt(grad_new_bf, hidden)
    dwab_ref[:, :width] += dot_lt(normed_bf, grad_a)
    dwab_ref[:, width:] += dot_lt(normed_bf, grad_b)
    grad_normed = dot_rt(grad_a, wpa_ref[...]) + dot_rt(grad_b, wpb_ref[...])
    dz_in = grad_new + norm_grad(normed, inv_std, grad_normed)
    dzin_ref[0] = dz_in.astype(BF16).reshape(ROWS, num_tok, chans)

    @pl.when(jnp.logical_and(pl.program_id(0) == pl.num_programs(0) - 1, step == pl.num_programs(1) - 1))
    def _():
        for g in range(width // LANES):
            rows, cols = slice(g * chans, (g + 1) * chans), slice(g * LANES, (g + 1) * LANES)
            pack_ref[0, rows, :] = dwab_ref[:, cols].astype(BF16)
            pack_ref[1, rows, :] = dwab_ref[:, width + g * LANES:width + (g + 1) * LANES].astype(BF16)
            pack_ref[2, rows, :] = dwot_ref[:, cols].astype(BF16)
        pack_ref[:, width:, :] = jnp.zeros((3, PAIR_ROWS - width, LANES), BF16)
        pack_ref[0, width:width + HEADS, :] = dwbt_ref[...].astype(BF16)


def single_kernel(idx_ref, own_ref, other_ref, mask_ref, ds_ref, bias_ref, wq_ref, qb_ref, wkv_ref, wg_ref, wo_ref, wsa_ref, wsb_ref, wso_ref,
                  pack_ref, dl_ref, send_ref, mid_ref, act_ref, full_scr, part_scr):
    idx = idx_ref[0]
    num_cplx, num_rows, chans = own_ref.shape

    def put(start, stop, values):
        for part in range(3):
            pack_ref[part, start:stop, :] = values[:, part * LANES:(part + 1) * LANES].astype(BF16)

    num_tok = 2 * num_rows
    for c in range(num_cplx):
        full_scr[pl.ds(pl.multiple_of(c * num_tok + idx * num_rows, 16), num_rows), :] = own_ref[c]
        full_scr[pl.ds(pl.multiple_of(c * num_tok + (1 - idx) * num_rows, 16), num_rows), :] = other_ref[c]
    s_own = own_ref[...].reshape(num_cplx * num_rows, chans)
    s_norm, s_inv = layer_norm(s_own)
    act = s_norm.astype(BF16)
    act_all = layer_norm(full_scr[...])[0].astype(BF16)
    queries = (dot(act, wq_ref[...]) + qb_ref[...].astype(F32)).astype(BF16)
    key_val = dot(act_all, wkv_ref[...]).astype(BF16)
    gate = sigmoid(dot(act, wg_ref[...]))
    lane = lax.broadcasted_iota(jnp.int32, (1, chans), 1)
    head_masks = [jnp.where((lane >= h * HEAD_DIM) & (lane < (h + 1) * HEAD_DIM), 1.0, 0.0) for h in range(HEADS)]

    def spread(values):
        return jnp.concatenate([values * head_masks[h].astype(BF16) for h in range(HEADS)], axis=0)

    def gather_heads(stacked):
        total = stacked[:num_rows] * head_masks[0]
        for h in range(1, HEADS):
            total += stacked[h * num_rows:(h + 1) * num_rows] * head_masks[h]
        return total

    probs, att_rows = [], []
    for c in range(num_cplx):
        keys = key_val[c * num_tok:(c + 1) * num_tok, :chans]
        values = key_val[c * num_tok:(c + 1) * num_tok, chans:]
        key_mask = MASK_BIG * (mask_ref[c:c + 1, :].astype(F32) - 1.0)
        logits = dot_rt(spread(queries[c * num_rows:(c + 1) * num_rows]), keys) * SCALE + bias_ref[c] + key_mask
        expo = jnp.exp(logits - jnp.max(logits, axis=-1, keepdims=True))
        prob = expo / jnp.sum(expo, axis=-1, keepdims=True)
        probs.append(prob)
        att_rows.append(gather_heads(dot(prob.astype(BF16), values)))
    attended = jnp.concatenate(att_rows, axis=0)
    gated = (gate * attended).astype(BF16)
    s_mid = (s_own.astype(F32) + dot(gated, wo_ref[...])).astype(BF16)
    mid_norm, mid_inv = layer_norm(s_mid)
    mid_act = mid_norm.astype(BF16)
    trans_a = dot(mid_act, wsa_ref[...])
    trans_b = dot(mid_act, wsb_ref[...])
    sig_a = sigmoid(trans_a)
    silu_a = trans_a * sig_a
    hidden = (silu_a * trans_b).astype(BF16)
    ds_rows = ds_ref[...].reshape(num_cplx * num_rows, chans)
    put(SO_AT, SA_AT, dot_lt(hidden, ds_rows))
    grad_hidden = dot_rt(ds_rows, wso_ref[...])
    grad_b = (grad_hidden * silu_a).astype(BF16)
    grad_a = (grad_hidden * trans_b * (sig_a + silu_a * (1.0 - sig_a))).astype(BF16)
    for part in range(4):
        cols = slice(part * chans, (part + 1) * chans)
        put(SA_AT + part * chans, SA_AT + (part + 1) * chans, dot_lt(mid_act, grad_a[:, cols]))
        put(SB_AT + part * chans, SB_AT + (part + 1) * chans, dot_lt(mid_act, grad_b[:, cols]))
    grad_mid_norm = dot_rt(grad_a, wsa_ref[...]) + dot_rt(grad_b, wsb_ref[...])
    grad_mid = ds_rows.astype(F32) + norm_grad(mid_norm, mid_inv, grad_mid_norm)
    mid_ref[...] = grad_mid
    grad_mid_bf = grad_mid.astype(BF16)
    put(O_AT, K_AT, dot_lt(gated, grad_mid_bf))
    grad_gated = dot_rt(grad_mid_bf, wo_ref[...])
    grad_gate = (grad_gated * attended * gate * (1.0 - gate)).astype(BF16)
    grad_att = (grad_gated * gate).astype(BF16)
    query_rows, key_rows, value_rows = [], [], []
    for c in range(num_cplx):
        keys = key_val[c * num_tok:(c + 1) * num_tok, :chans]
        values = key_val[c * num_tok:(c + 1) * num_tok, chans:]
        prob = probs[c]
        att_spread = spread(grad_att[c * num_rows:(c + 1) * num_rows])
        grad_prob = dot_rt(att_spread, values)
        value_rows.append(dot_lt(prob.astype(BF16), att_spread))
        grad_logits = prob * (grad_prob - jnp.sum(prob * grad_prob, axis=-1, keepdims=True))
        grad_bf = grad_logits.astype(BF16)
        dl_ref[c] = grad_bf.astype(F32)
        query_rows.append(gather_heads(dot(grad_bf, keys)) * SCALE)
        key_rows.append(dot_lt(grad_bf, spread(queries[c * num_rows:(c + 1) * num_rows])) * SCALE)
    grad_query = jnp.concatenate(query_rows, axis=0)
    grad_query_bf = grad_query.astype(BF16)
    grad_key_bf = jnp.concatenate(key_rows, axis=0).astype(BF16)
    grad_value_bf = jnp.concatenate(value_rows, axis=0).astype(BF16)
    put(Q_AT, G_AT, dot_lt(act, grad_query_bf))
    put(G_AT, O_AT, dot_lt(act, grad_gate))
    put(K_AT, V_AT, dot_lt(act_all, grad_key_bf))
    put(V_AT, SO_AT, dot_lt(act_all, grad_value_bf))
    row = lax.broadcasted_iota(jnp.int32, (PACK_ROWS - QB_AT, 1), 0)
    put(QB_AT, PACK_ROWS, jnp.where(row == 0, jnp.sum(grad_query, axis=0, keepdims=True), 0.0))
    part_scr[...] = dot_rt(grad_key_bf, wkv_ref[:, :chans]) + dot_rt(grad_value_bf, wkv_ref[:, chans:])
    local = dot_rt(grad_query_bf, wq_ref[...]) + dot_rt(grad_gate, wg_ref[...])
    for c in range(num_cplx):
        rows = slice(c * num_rows, (c + 1) * num_rows)
        act_ref[rows, :] = local[rows] + part_scr[pl.ds(pl.multiple_of(c * num_tok + idx * num_rows, 8), num_rows), :]
        send_ref[rows, :] = part_scr[pl.ds(pl.multiple_of(c * num_tok + (1 - idx) * num_rows, 8), num_rows), :].astype(BF16)


def finish_kernel(own_ref, mid_ref, act_ref, recv_ref, pack_ref, pair_ref, out_ref,
                  pa_ref, pb_ref, po_ref, bias_ref, q_ref, qb_ref, kv_ref, g_ref, o_ref, sa_ref, sb_ref, so_ref):
    s_norm, s_inv = layer_norm(own_ref[...])
    grad_act = act_ref[...] + recv_ref[...].astype(F32)
    out_ref[...] = (mid_ref[...] + norm_grad(s_norm, s_inv, grad_act)).astype(BF16)
    chans = po_ref.shape[1]
    width = po_ref.shape[0]
    for g in range(width // LANES):
        rows, cols = slice(g * chans, (g + 1) * chans), slice(g * LANES, (g + 1) * LANES)
        pa_ref[:, cols] = pair_ref[0, rows, :].astype(F32)
        pb_ref[:, cols] = pair_ref[1, rows, :].astype(F32)
        po_ref[cols, :] = pair_ref[2, rows, :].astype(F32).T
    bias_ref[...] = pair_ref[0, width:width + HEADS, :].astype(F32)
    side = q_ref.shape[0]
    for p in range(3):
        cols = slice(p * LANES, (p + 1) * LANES)
        q_ref[:, cols] = pack_ref[p, Q_AT:G_AT, :].astype(F32)
        g_ref[:, cols] = pack_ref[p, G_AT:O_AT, :].astype(F32)
        o_ref[:, cols] = pack_ref[p, O_AT:K_AT, :].astype(F32)
        qb_ref[:, cols] = pack_ref[p, QB_AT:QB_AT + 16, :].astype(F32)[:1]
        so_ref[:, cols] = pack_ref[p, SO_AT:SA_AT, :].astype(F32)
        for part in range(4):
            wide = slice(part * side + p * LANES, part * side + (p + 1) * LANES)
            if part < 2:
                kv_ref[:, wide] = pack_ref[p, K_AT + part * side:K_AT + (part + 1) * side, :].astype(F32)
            sa_ref[:, wide] = pack_ref[p, SA_AT + part * side:SA_AT + (part + 1) * side, :].astype(F32)
            sb_ref[:, wide] = pack_ref[p, SB_AT + part * side:SB_AT + (part + 1) * side, :].astype(F32)


STRIDES = (1, 4, 16)
ORDERS = ((0, 1, 2), (1, 2, 0), (2, 0, 1))
RING = 4


def reduce_scratch(rows, scatter):
    half = rows // 2
    long = half // RING
    short = long // RING if scatter else long
    return [
        pltpu.VMEM((3, half, LANES), BF16),
        pltpu.VMEM((3, half, LANES), BF16),
        pltpu.VMEM((3, RING - 1, long, LANES), BF16),
        pltpu.VMEM((3, RING, short, LANES), BF16),
        pltpu.VMEM((3, RING, short, LANES), BF16),
        pltpu.VMEM((3, long, LANES), BF16),
        pltpu.VMEM((3, long, LANES), BF16),
        pltpu.SemaphoreType.DMA((2, 2, 3)),
        pltpu.SemaphoreType.DMA((2, 5, 3, RING - 1)),
    ]


NUM_REDUCE = 9


class Reduce:
    def __init__(self, in_ref, out_ref, scratch, scatter):
        self.src, self.out, self.scatter = in_ref, out_ref, scatter
        self.got, self.half, self.long_got, self.mid, self.last, self.long, self.whole, self.pair_sem, self.sem = scratch
        self.half_rows = self.half.shape[1]
        self.long_rows = self.long.shape[1]
        self.short_rows = self.mid.shape[2]
        self.block = self.short_rows
        self.core = lax.axis_index('dap')
        self.dp = lax.axis_index('dp')

    def coord(self, part, phase):
        return (self.dp // STRIDES[ORDERS[part][phase]]) % RING

    def pair_copy(self, part, which):
        if which == 0:
            src = self.src.at[part, pl.ds(pl.multiple_of((1 - self.core) * self.half_rows, 16), self.half_rows), :]
            dst = self.got.at[part]
        else:
            src = dst = self.out.at[part, pl.ds(pl.multiple_of(self.core * self.half_rows, 16), self.half_rows), :]
        return pltpu.make_async_remote_copy(src_ref=src, dst_ref=dst, send_sem=self.pair_sem.at[0, which, part], recv_sem=self.pair_sem.at[1, which, part],
                                            device_id={'dap': 1 - self.core}, device_id_type=MESH)

    def ring_copy(self, part, leg, offset):
        axis = ORDERS[part][(0, 1, 2, 1, 0)[leg]]
        here = (self.dp // STRIDES[axis]) % RING
        peer = (here + offset) % RING
        if leg == 0:
            src = self.half.at[part, pl.ds(pl.multiple_of(peer * self.long_rows, 16), self.long_rows), :]
            dst = self.long_got.at[part, offset - 1]
        elif leg == 1 and self.scatter:
            src = self.long.at[part, pl.ds(pl.multiple_of(peer * self.short_rows, 16), self.short_rows), :]
            dst = self.mid.at[part, offset - 1]
        elif leg == 1:
            src = dst = self.mid.at[part, here]
        elif leg == 2:
            src = dst = self.last.at[part, here]
        elif leg == 3:
            src = dst = self.whole.at[part, pl.ds(pl.multiple_of(here * self.short_rows, 16), self.short_rows), :]
        else:
            rows = pl.ds(pl.multiple_of(self.core * self.half_rows + here * self.long_rows, 16), self.long_rows)
            src = dst = self.out.at[part, rows, :]
        return pltpu.make_async_remote_copy(src_ref=src, dst_ref=dst, send_sem=self.sem.at[0, leg, part, offset - 1], recv_sem=self.sem.at[1, leg, part, offset - 1],
                                            device_id={'dp': self.dp + (peer - here) * STRIDES[axis]}, device_id_type=MESH)

    def send(self, part, leg):
        for offset in range(1, RING):
            self.ring_copy(part, leg, offset).start()

    def arrive(self, part, leg):
        for offset in range(1, RING):
            self.ring_copy(part, leg, offset).wait_recv()

    def add(self, rows, put, gets):
        def step(i, carry):
            at = pl.multiple_of(i * self.block, 16)
            total = gets[0](at).astype(F32)
            for get in gets[1:]:
                total += get(at).astype(F32)
            put(at, total.astype(BF16))
            return carry

        lax.fori_loop(0, rows // self.block, step, 0)

    def reader(self, ref, *lead, base=0):
        return lambda at: ref[(*lead, pl.ds(pl.multiple_of(base + at, 16), self.block), slice(None))]

    def writer(self, ref, *lead, base=0):
        def put(at, values):
            ref[(*lead, pl.ds(pl.multiple_of(base + at, 16), self.block), slice(None))] = values
        return put

    def start(self):
        for part in range(3):
            self.pair_copy(part, 0).start()

    def step(self, number):
        for part in range(3):
            self.part_step(number, part)

    def part_step(self, number, part):
        half, long, short = self.half_rows, self.long_rows, self.short_rows
        if number == 0:
            self.pair_copy(part, 0).wait_recv()
            self.add(half, self.writer(self.half, part), [self.reader(self.src, part, base=self.core * half), self.reader(self.got, part)])
            self.send(part, 0)
        elif number == 1:
            self.arrive(part, 0)
            gets = [self.reader(self.half, part, base=self.coord(part, 0) * long)] + [self.reader(self.long_got, part, i) for i in range(RING - 1)]
            put = self.writer(self.long, part) if self.scatter else self.writer(self.mid, part, self.coord(part, 1))
            self.add(long, put, gets)
            self.send(part, 1)
        elif number == 2:
            self.arrive(part, 1)
            if self.scatter:
                gets = [self.reader(self.long, part, base=self.coord(part, 1) * short)] + [self.reader(self.mid, part, i) for i in range(RING - 1)]
            else:
                gets = [self.reader(self.mid, part, i) for i in range(RING)]
            self.add(short, self.writer(self.last, part, self.coord(part, 2)), gets)
            self.send(part, 2)
        elif number == 3:
            self.arrive(part, 2)
            gets = [self.reader(self.last, part, i) for i in range(RING)]
            if self.scatter:
                self.add(short, self.writer(self.whole, part, base=self.coord(part, 1) * short), gets)
                self.send(part, 3)
            else:
                self.add(short, self.writer(self.out, part, base=self.core * half + self.coord(part, 0) * long), gets)
                self.send(part, 4)
        elif number == 4 and self.scatter:
            self.arrive(part, 3)
            self.add(long, self.writer(self.out, part, base=self.core * half + self.coord(part, 0) * long), [self.reader(self.whole, part)])
            self.send(part, 4)
        elif number == 5:
            self.arrive(part, 4)
            self.pair_copy(part, 1).start()
        elif number == 6:
            self.pair_copy(part, 1).wait_recv()
            for which in range(2):
                self.pair_copy(part, which).wait_send()
            for leg in range(5):
                if leg != 3 or self.scatter:
                    for offset in range(1, RING):
                        self.ring_copy(part, leg, offset).wait_send()


NUM_STEPS = 7


def enter_barrier():
    barrier = pltpu.get_barrier_semaphore()
    dp = lax.axis_index('dp')
    pl.semaphore_signal(barrier, inc=1, device_id={'dap': 1 - lax.axis_index('dap')}, device_id_type=MESH)
    for stride in STRIDES:
        here = (dp // stride) % RING
        for offset in range(1, RING):
            pl.semaphore_signal(barrier, inc=1, device_id={'dp': dp + ((here + offset) % RING - here) * stride}, device_id_type=MESH)
    pl.semaphore_wait(barrier, 1 + 3 * (RING - 1))


def reduce_kernel(pack_ref, pair_ref, pack_out, pair_out, *scratch):
    enter_barrier()
    sums = [Reduce(pair_ref, pair_out, scratch[NUM_REDUCE:], False), Reduce(pack_ref, pack_out, scratch[:NUM_REDUCE], True)]
    for one in sums:
        one.start()
    for number in range(NUM_STEPS):
        for one in sums:
            one.step(number)


VMEM_LIMIT = 60 * 1024 * 1024


def solution(mesh):
    pair_spec = P('dp', 'dap', None, None)
    single_spec = P('dp', 'dap', None)

    def body(pair_z, single_s, token_mask, dz_out, ds_out, w_pa, w_pb, w_po, w_bias, w_q, q_bias, w_kv, w_g, w_o, w_sa, w_sb, w_so):
        num_cplx, num_rows, num_tok, chans = pair_z.shape
        s_chans = single_s.shape[2]
        width = w_pa.shape[1]
        idx = lax.axis_index('dap')
        swap = [(0, 1), (1, 0)]
        other_s = lax.ppermute(single_s, 'dap', swap)
        w_bias_t = w_bias.T
        steps = num_rows // ROWS
        row_spec = pl.BlockSpec((1, ROWS, num_tok, chans), lambda c, r: (c, r, 0, 0))
        head_spec = pl.BlockSpec((1, HEADS * num_rows, num_tok), lambda c, r: (c, 0, 0))

        def whole(shape):
            return pl.BlockSpec(shape, lambda c, r: (0,) * len(shape))

        positions = num_cplx * num_rows * num_tok
        z_new, bias = pl.pallas_call(
            pair_forward_kernel,
            grid=(num_cplx, steps),
            in_specs=[row_spec, whole(w_pa.shape), whole(w_pb.shape), whole(w_po.shape), whole(w_bias_t.shape)],
            out_specs=[row_spec, head_spec],
            out_shape=[jax.ShapeDtypeStruct(pair_z.shape, BF16), jax.ShapeDtypeStruct((num_cplx, HEADS * num_rows, num_tok), F32)],
            compiler_params=pltpu.CompilerParams(dimension_semantics=('arbitrary', 'arbitrary'), vmem_limit_bytes=VMEM_LIMIT),
            cost_estimate=pl.CostEstimate(flops=positions * 3 * 2 * chans * width, bytes_accessed=positions * chans * 4, transcendentals=positions * width),
            name='pair_forward',
        )(pair_z, w_pa, w_pb, w_po, w_bias_t)

        tokens = num_cplx * num_rows
        pack, d_logits, send, grad_mid, grad_act = pl.pallas_call(
            single_kernel,
            in_specs=[pl.BlockSpec(memory_space=pltpu.SMEM)] + [pl.BlockSpec(memory_space=pltpu.VMEM)] * 13,
            out_specs=[pl.BlockSpec(memory_space=pltpu.VMEM)] * 5,
            out_shape=[
                jax.ShapeDtypeStruct((3, PACK_ROWS, LANES), BF16),
                jax.ShapeDtypeStruct((num_cplx, HEADS * num_rows, num_tok), F32),
                jax.ShapeDtypeStruct((tokens, s_chans), BF16),
                jax.ShapeDtypeStruct((tokens, s_chans), F32),
                jax.ShapeDtypeStruct((tokens, s_chans), F32),
            ],
            scratch_shapes=[pltpu.VMEM((2 * tokens, s_chans), BF16), pltpu.VMEM((2 * tokens, s_chans), F32)],
            compiler_params=pltpu.CompilerParams(vmem_limit_bytes=VMEM_LIMIT),
            cost_estimate=pl.CostEstimate(flops=10 ** 10, bytes_accessed=10 ** 7, transcendentals=10 ** 6),
            name='single_path',
        )(idx.reshape(1).astype(jnp.int32), single_s, other_s, token_mask, ds_out, bias, w_q, q_bias.reshape(1, s_chans), w_kv, w_g, w_o, w_sa, w_sb, w_so)

        recv = lax.ppermute(send, 'dap', swap)

        dz_in, pair_pack = pl.pallas_call(
            pair_backward_kernel,
            grid=(num_cplx, steps),
            in_specs=[row_spec, row_spec, row_spec, head_spec, whole(w_pa.shape), whole(w_pb.shape), whole(w_po.shape), whole(w_bias_t.shape)],
            out_specs=[row_spec, whole((3, PAIR_ROWS, LANES))],
            out_shape=[
                jax.ShapeDtypeStruct(pair_z.shape, BF16),
                jax.ShapeDtypeStruct((3, PAIR_ROWS, LANES), BF16),
            ],
            scratch_shapes=[pltpu.VMEM((chans, 2 * width), F32), pltpu.VMEM((chans, width), F32), pltpu.VMEM(w_bias_t.shape, F32)],
            compiler_params=pltpu.CompilerParams(dimension_semantics=('arbitrary', 'arbitrary'), vmem_limit_bytes=VMEM_LIMIT),
            cost_estimate=pl.CostEstimate(flops=positions * 8 * 2 * chans * width, bytes_accessed=positions * chans * 8, transcendentals=positions * width),
            name='pair_backward',
        )(pair_z, z_new, dz_out, d_logits, w_pa, w_pb, w_po, w_bias_t)

        pack, pair_pack = pl.pallas_call(
            reduce_kernel,
            in_specs=[pl.BlockSpec(memory_space=pltpu.VMEM)] * 2,
            out_specs=[pl.BlockSpec(memory_space=pltpu.VMEM)] * 2,
            out_shape=[jax.ShapeDtypeStruct(pack.shape, BF16), jax.ShapeDtypeStruct(pair_pack.shape, BF16)],
            scratch_shapes=reduce_scratch(PACK_ROWS, True) + reduce_scratch(PAIR_ROWS, False),
            compiler_params=pltpu.CompilerParams(vmem_limit_bytes=VMEM_LIMIT, collective_id=0, has_side_effects=True),
            cost_estimate=pl.CostEstimate(flops=10 ** 9, bytes_accessed=2 * 10 ** 7, transcendentals=0),
            name='sum_grads',
        )(pack, pair_pack)

        grad_shapes = [w_pa.shape, w_pb.shape, w_po.shape, w_bias_t.shape, w_q.shape, (1, s_chans), w_kv.shape, w_g.shape, w_o.shape, w_sa.shape, w_sb.shape, w_so.shape]
        outs = pl.pallas_call(
            finish_kernel,
            in_specs=[pl.BlockSpec(memory_space=pltpu.VMEM)] * 6,
            out_specs=[pl.BlockSpec(memory_space=pltpu.VMEM)] * 13,
            out_shape=[jax.ShapeDtypeStruct((tokens, s_chans), BF16)] + [jax.ShapeDtypeStruct(shape, F32) for shape in grad_shapes],
            compiler_params=pltpu.CompilerParams(vmem_limit_bytes=VMEM_LIMIT),
            name='finish',
        )(single_s.reshape(tokens, s_chans), grad_mid, grad_act, recv, pack, pair_pack)
        ds_in = outs[0].reshape(single_s.shape)
        grads = list(outs[1:])
        grads[3] = grads[3].T
        grads[5] = grads[5].reshape(s_chans)
        return (dz_in, ds_in, *grads)

    in_specs = (pair_spec, single_spec, P('dp', None), pair_spec, single_spec) + (P(),) * 12
    out_specs = (pair_spec, single_spec) + (P(),) * 12
    return jax.shard_map(body, mesh=mesh, in_specs=in_specs, out_specs=out_specs, check_vma=False)
```

```python
import functools
import jax
import jax.numpy as jnp
from jax import lax
from jax.experimental import pallas as pl
from jax.experimental.pallas import tpu as pltpu
from jax.sharding import PartitionSpec as P

HEADS = 16
HEAD_DIM = 24
EPSILON = 1e-5
MASK_BIG = 1e9
SCALE = HEAD_DIM ** -0.5
ROWS = 8
LANES = 128
PAIR_ROWS = 640
MESH = pl.DeviceIdType.MESH
F32 = jnp.float32
BF16 = jnp.bfloat16

Q_AT, G_AT, O_AT, K_AT, V_AT, SO_AT, SA_AT, SB_AT, QB_AT, PACK_ROWS = 0, 384, 768, 1152, 1536, 1920, 3456, 4992, 6528, 6656


def dot(left, right):
    return lax.dot_general(left, right, (((1,), (0,)), ((), ())), preferred_element_type=F32)


def dot_rt(left, right):
    return lax.dot_general(left, right, (((1,), (1,)), ((), ())), preferred_element_type=F32)


def dot_lt(left, right):
    return lax.dot_general(left, right, (((0,), (0,)), ((), ())), preferred_element_type=F32)


def layer_norm(values):
    wide = values.astype(F32)
    centred = wide - jnp.mean(wide, axis=-1, keepdims=True)
    inv_std = lax.rsqrt(jnp.mean(centred * centred, axis=-1, keepdims=True) + EPSILON)
    return centred * inv_std, inv_std


def norm_grad(normed, inv_std, grad_out):
    mean_grad = jnp.mean(grad_out, axis=-1, keepdims=True)
    mean_proj = jnp.mean(grad_out * normed, axis=-1, keepdims=True)
    return inv_std * (grad_out - mean_grad - normed * mean_proj)


def sigmoid(values):
    return jax.nn.sigmoid(values)


def pair_forward_kernel(z_ref, wpa_ref, wpb_ref, wpo_ref, wbt_ref, znew_ref, bias_ref):
    step = pl.program_id(1)
    num_tok = z_ref.shape[2]
    num_rows = bias_ref.shape[1] // HEADS
    z_rows = z_ref[0].reshape(ROWS * num_tok, z_ref.shape[3])
    normed, _ = layer_norm(z_rows)
    normed_bf = normed.astype(BF16)
    hid_a, hid_b = dot(normed_bf, wpa_ref[...]), dot(normed_bf, wpb_ref[...])
    hidden = (hid_a * sigmoid(hid_a) * hid_b).astype(BF16)
    z_new = (z_rows.astype(F32) + dot(hidden, wpo_ref[...])).astype(BF16)
    znew_ref[0] = z_new.reshape(ROWS, num_tok, z_new.shape[1])
    bias_norm, _ = layer_norm(z_new)
    bias_bf = bias_norm.astype(BF16)
    for r in range(ROWS):
        bias_ref[0, pl.ds(step * ROWS + r, HEADS, stride=num_rows), :] = dot_rt(wbt_ref[...], bias_bf[r * num_tok:(r + 1) * num_tok])


def backward_kernel(z_ref, znew_ref, dz_ref, dl_ref, wpa_ref, wpb_ref, wpo_ref, wbt_ref, pack_ref, dzin_ref, sum_ref, pair_ref,
                    dwa_ref, dwb_ref, dwot_ref, dwbt_ref, pair_pack, ga_ref, gb_ref, gnew_ref, *scratch):
    second, step = pl.program_id(0), pl.program_id(1)
    num_steps = pl.num_programs(1)
    num_tok, chans = z_ref.shape[2], z_ref.shape[3]
    num_rows = dl_ref.shape[1] // HEADS
    width = wpo_ref.shape[0]
    flat = (ROWS * num_tok, chans)
    tick = second * num_steps + step
    single_sum = Reduce(pack_ref, sum_ref, scratch[:NUM_REDUCE], True)
    pair_sum = Reduce(pair_pack, pair_ref, scratch[NUM_REDUCE:], False)

    @pl.when(tick == 0)
    def _():
        dwa_ref[...] = jnp.zeros_like(dwa_ref)
        dwb_ref[...] = jnp.zeros_like(dwb_ref)
        dwot_ref[...] = jnp.zeros_like(dwot_ref)
        dwbt_ref[...] = jnp.zeros_like(dwbt_ref)
        enter_barrier()
        single_sum.start()

    for one, ticks in ((single_sum, SINGLE_TICKS), (pair_sum, PAIR_TICKS)):
        for number, at in enumerate(ticks):
            @pl.when(tick == at)
            def _(one=one, number=number):
                one.step(number)

    @pl.when(second == 0)
    def _():
        bias_norm, bias_inv = layer_norm(znew_ref[0].reshape(flat))
        bias_bf = bias_norm.astype(BF16)
        grad_rows = []
        d_bias_t = jnp.zeros(dwbt_ref.shape, F32)
        first = lax.rem(step, num_rows // ROWS) * ROWS
        for r in range(ROWS):
            dl_row = dl_ref[0, pl.ds(first + r, HEADS, stride=num_rows), :].astype(BF16)
            grad_rows.append(dot_lt(dl_row, wbt_ref[...]))
            d_bias_t += dot(dl_row, bias_bf[r * num_tok:(r + 1) * num_tok])
        dwbt_ref[...] += d_bias_t
        grad_norm = jnp.concatenate(grad_rows, axis=0)
        grad_new = dz_ref[0].reshape(flat).astype(F32) + norm_grad(bias_norm, bias_inv, grad_norm)
        grad_new_bf = grad_new.astype(BF16)
        gnew_ref[step] = grad_new_bf
        normed, _ = layer_norm(z_ref[0].reshape(flat))
        normed_bf = normed.astype(BF16)
        hid_a, hid_b = dot(normed_bf, wpa_ref[...]), dot(normed_bf, wpb_ref[...])
        grad_hidden = dot_rt(grad_new_bf, wpo_ref[...])
        sig_a = sigmoid(hid_a)
        silu_a = hid_a * sig_a
        hidden = (silu_a * hid_b).astype(BF16)
        grad_b = (grad_hidden * silu_a).astype(BF16)
        grad_a = (grad_hidden * hid_b * (sig_a + silu_a * (1.0 - sig_a))).astype(BF16)
        ga_ref[step] = grad_a
        gb_ref[step] = grad_b
        dwot_ref[...] += dot_lt(grad_new_bf, hidden)
        dwa_ref[...] += dot_lt(normed_bf, grad_a)
        dwb_ref[...] += dot_lt(normed_bf, grad_b)

    @pl.when(tick == num_steps - 1)
    def _():
        for g in range(width // LANES):
            rows, cols = slice(g * chans, (g + 1) * chans), slice(g * LANES, (g + 1) * LANES)
            pair_pack[0, rows, :] = dwa_ref[:, cols].astype(BF16)
            pair_pack[1, rows, :] = dwb_ref[:, cols].astype(BF16)
            pair_pack[2, rows, :] = dwot_ref[:, cols].astype(BF16)
        pair_pack[:, width:, :] = jnp.zeros((3, PAIR_ROWS - width, LANES), BF16)
        pair_pack[0, width:width + HEADS, :] = dwbt_ref[...].astype(BF16)
        pair_sum.start()

    @pl.when(second == 1)
    def _():
        normed, inv_std = layer_norm(z_ref[0].reshape(flat))
        grad_normed = dot_rt(ga_ref[step], wpa_ref[...]) + dot_rt(gb_ref[step], wpb_ref[...])
        dz_in = gnew_ref[step].astype(F32) + norm_grad(normed, inv_std, grad_normed)
        dzin_ref[0] = dz_in.astype(BF16).reshape(ROWS, num_tok, chans)

    @pl.when(tick == 2 * num_steps - 1)
    def _():
        pair_sum.step(NUM_STEPS - 1)
        single_sum.step(NUM_STEPS - 1)


SINGLE_TICKS = (3, 9, 12, 14, 17, 31)
PAIR_TICKS = (20, 23, 26, 29, 30, 33)


def single_kernel(idx_ref, own_ref, other_ref, mask_ref, ds_ref, bias_ref, wq_ref, qb_ref, wkv_ref, wg_ref, wo_ref, wsa_ref, wsb_ref, wso_ref,
                  pack_ref, dl_ref, send_ref, mid_ref, act_ref, full_scr, part_scr):
    idx = idx_ref[0]
    num_cplx, num_rows, chans = own_ref.shape

    def put(start, stop, values):
        for part in range(3):
            pack_ref[part, start:stop, :] = values[:, part * LANES:(part + 1) * LANES].astype(BF16)

    num_tok = 2 * num_rows
    for c in range(num_cplx):
        full_scr[pl.ds(pl.multiple_of(c * num_tok + idx * num_rows, 16), num_rows), :] = own_ref[c]
        full_scr[pl.ds(pl.multiple_of(c * num_tok + (1 - idx) * num_rows, 16), num_rows), :] = other_ref[c]
    s_own = own_ref[...].reshape(num_cplx * num_rows, chans)
    s_norm, s_inv = layer_norm(s_own)
    act = s_norm.astype(BF16)
    act_all = layer_norm(full_scr[...])[0].astype(BF16)
    queries = (dot(act, wq_ref[...]) + qb_ref[...].astype(F32)).astype(BF16)
    key_val = dot(act_all, wkv_ref[...]).astype(BF16)
    gate = sigmoid(dot(act, wg_ref[...]))
    lane = lax.broadcasted_iota(jnp.int32, (1, chans), 1)
    head_masks = [jnp.where((lane >= h * HEAD_DIM) & (lane < (h + 1) * HEAD_DIM), 1.0, 0.0) for h in range(HEADS)]

    def spread(values):
        return jnp.concatenate([values * head_masks[h].astype(BF16) for h in range(HEADS)], axis=0)

    def gather_heads(stacked):
        total = stacked[:num_rows] * head_masks[0]
        for h in range(1, HEADS):
            total += stacked[h * num_rows:(h + 1) * num_rows] * head_masks[h]
        return total

    probs, att_rows = [], []
    for c in range(num_cplx):
        keys = key_val[c * num_tok:(c + 1) * num_tok, :chans]
        values = key_val[c * num_tok:(c + 1) * num_tok, chans:]
        key_mask = MASK_BIG * (mask_ref[c:c + 1, :].astype(F32) - 1.0)
        logits = dot_rt(spread(queries[c * num_rows:(c + 1) * num_rows]), keys) * SCALE + bias_ref[c] + key_mask
        expo = jnp.exp(logits - jnp.max(logits, axis=-1, keepdims=True))
        prob = expo / jnp.sum(expo, axis=-1, keepdims=True)
        probs.append(prob)
        att_rows.append(gather_heads(dot(prob.astype(BF16), values)))
    attended = jnp.concatenate(att_rows, axis=0)
    gated = (gate * attended).astype(BF16)
    s_mid = (s_own.astype(F32) + dot(gated, wo_ref[...])).astype(BF16)
    mid_norm, mid_inv = layer_norm(s_mid)
    mid_act = mid_norm.astype(BF16)
    trans_a = dot(mid_act, wsa_ref[...])
    trans_b = dot(mid_act, wsb_ref[...])
    sig_a = sigmoid(trans_a)
    silu_a = trans_a * sig_a
    hidden = (silu_a * trans_b).astype(BF16)
    ds_rows = ds_ref[...].reshape(num_cplx * num_rows, chans)
    put(SO_AT, SA_AT, dot_lt(hidden, ds_rows))
    grad_hidden = dot_rt(ds_rows, wso_ref[...])
    grad_b = (grad_hidden * silu_a).astype(BF16)
    grad_a = (grad_hidden * trans_b * (sig_a + silu_a * (1.0 - sig_a))).astype(BF16)
    for part in range(4):
        cols = slice(part * chans, (part + 1) * chans)
        put(SA_AT + part * chans, SA_AT + (part + 1) * chans, dot_lt(mid_act, grad_a[:, cols]))
        put(SB_AT + part * chans, SB_AT + (part + 1) * chans, dot_lt(mid_act, grad_b[:, cols]))
    grad_mid_norm = dot_rt(grad_a, wsa_ref[...]) + dot_rt(grad_b, wsb_ref[...])
    grad_mid = ds_rows.astype(F32) + norm_grad(mid_norm, mid_inv, grad_mid_norm)
    mid_ref[...] = grad_mid
    grad_mid_bf = grad_mid.astype(BF16)
    put(O_AT, K_AT, dot_lt(gated, grad_mid_bf))
    grad_gated = dot_rt(grad_mid_bf, wo_ref[...])
    grad_gate = (grad_gated * attended * gate * (1.0 - gate)).astype(BF16)
    grad_att = (grad_gated * gate).astype(BF16)
    query_rows, key_rows, value_rows = [], [], []
    for c in range(num_cplx):
        keys = key_val[c * num_tok:(c + 1) * num_tok, :chans]
        values = key_val[c * num_tok:(c + 1) * num_tok, chans:]
        prob = probs[c]
        att_spread = spread(grad_att[c * num_rows:(c + 1) * num_rows])
        grad_prob = dot_rt(att_spread, values)
        value_rows.append(dot_lt(prob.astype(BF16), att_spread))
        grad_logits = prob * (grad_prob - jnp.sum(prob * grad_prob, axis=-1, keepdims=True))
        grad_bf = grad_logits.astype(BF16)
        dl_ref[c] = grad_bf.astype(F32)
        query_rows.append(gather_heads(dot(grad_bf, keys)) * SCALE)
        key_rows.append(dot_lt(grad_bf, spread(queries[c * num_rows:(c + 1) * num_rows])) * SCALE)
    grad_query = jnp.concatenate(query_rows, axis=0)
    grad_query_bf = grad_query.astype(BF16)
    grad_key_bf = jnp.concatenate(key_rows, axis=0).astype(BF16)
    grad_value_bf = jnp.concatenate(value_rows, axis=0).astype(BF16)
    put(Q_AT, G_AT, dot_lt(act, grad_query_bf))
    put(G_AT, O_AT, dot_lt(act, grad_gate))
    put(K_AT, V_AT, dot_lt(act_all, grad_key_bf))
    put(V_AT, SO_AT, dot_lt(act_all, grad_value_bf))
    row = lax.broadcasted_iota(jnp.int32, (PACK_ROWS - QB_AT, 1), 0)
    put(QB_AT, PACK_ROWS, jnp.where(row == 0, jnp.sum(grad_query, axis=0, keepdims=True), 0.0))
    part_scr[...] = dot_rt(grad_key_bf, wkv_ref[:, :chans]) + dot_rt(grad_value_bf, wkv_ref[:, chans:])
    local = dot_rt(grad_query_bf, wq_ref[...]) + dot_rt(grad_gate, wg_ref[...])
    for c in range(num_cplx):
        rows = slice(c * num_rows, (c + 1) * num_rows)
        act_ref[rows, :] = local[rows] + part_scr[pl.ds(pl.multiple_of(c * num_tok + idx * num_rows, 8), num_rows), :]
        send_ref[rows, :] = part_scr[pl.ds(pl.multiple_of(c * num_tok + (1 - idx) * num_rows, 8), num_rows), :].astype(BF16)


def finish_kernel(own_ref, mid_ref, act_ref, recv_ref, pack_ref, pair_ref, out_ref,
                  pa_ref, pb_ref, po_ref, bias_ref, q_ref, qb_ref, kv_ref, g_ref, o_ref, sa_ref, sb_ref, so_ref):
    s_norm, s_inv = layer_norm(own_ref[...])
    grad_act = act_ref[...] + recv_ref[...].astype(F32)
    out_ref[...] = (mid_ref[...] + norm_grad(s_norm, s_inv, grad_act)).astype(BF16)
    chans = po_ref.shape[1]
    width = po_ref.shape[0]
    for g in range(width // LANES):
        rows, cols = slice(g * chans, (g + 1) * chans), slice(g * LANES, (g + 1) * LANES)
        pa_ref[:, cols] = pair_ref[0, rows, :].astype(F32)
        pb_ref[:, cols] = pair_ref[1, rows, :].astype(F32)
        po_ref[cols, :] = pair_ref[2, rows, :].astype(F32).T
    bias_ref[...] = pair_ref[0, width:width + HEADS, :].astype(F32)
    side = q_ref.shape[0]
    for p in range(3):
        cols = slice(p * LANES, (p + 1) * LANES)
        q_ref[:, cols] = pack_ref[p, Q_AT:G_AT, :].astype(F32)
        g_ref[:, cols] = pack_ref[p, G_AT:O_AT, :].astype(F32)
        o_ref[:, cols] = pack_ref[p, O_AT:K_AT, :].astype(F32)
        qb_ref[:, cols] = pack_ref[p, QB_AT:QB_AT + 16, :].astype(F32)[:1]
        so_ref[:, cols] = pack_ref[p, SO_AT:SA_AT, :].astype(F32)
        for part in range(4):
            wide = slice(part * side + p * LANES, part * side + (p + 1) * LANES)
            if part < 2:
                kv_ref[:, wide] = pack_ref[p, K_AT + part * side:K_AT + (part + 1) * side, :].astype(F32)
            sa_ref[:, wide] = pack_ref[p, SA_AT + part * side:SA_AT + (part + 1) * side, :].astype(F32)
            sb_ref[:, wide] = pack_ref[p, SB_AT + part * side:SB_AT + (part + 1) * side, :].astype(F32)


STRIDES = (1, 4, 16)
ORDERS = ((0, 1, 2), (1, 2, 0), (2, 0, 1))
RING = 4


def reduce_scratch(rows, scatter):
    half = rows // 2
    long = half // RING
    short = long // RING if scatter else long
    return [
        pltpu.VMEM((3, half, LANES), BF16),
        pltpu.VMEM((3, half, LANES), BF16),
        pltpu.VMEM((3, RING - 1, long, LANES), BF16),
        pltpu.VMEM((3, RING, short, LANES), BF16),
        pltpu.VMEM((3, RING, short, LANES), BF16),
        pltpu.VMEM((3, long, LANES), BF16),
        pltpu.VMEM((3, long, LANES), BF16),
        pltpu.SemaphoreType.DMA((2, 2, 3)),
        pltpu.SemaphoreType.DMA((2, 5, 3, RING - 1)),
        pltpu.SemaphoreType.DMA((2, 3)),
    ]


NUM_REDUCE = 10


class Reduce:
    def __init__(self, in_ref, out_ref, scratch, scatter):
        self.src, self.out, self.scatter = in_ref, out_ref, scatter
        self.got, self.half, self.long_got, self.mid, self.last, self.long, self.whole, self.pair_sem, self.sem, self.own_sem = scratch
        self.half_rows = self.half.shape[1]
        self.long_rows = self.long.shape[1]
        self.short_rows = self.mid.shape[2]
        self.block = self.short_rows
        self.core = lax.axis_index('dap')
        self.dp = lax.axis_index('dp')

    def coord(self, part, phase):
        return (self.dp // STRIDES[ORDERS[part][phase]]) % RING

    def pair_copy(self, part, which):
        if which == 0:
            src = self.src.at[part, pl.ds(pl.multiple_of((1 - self.core) * self.half_rows, 16), self.half_rows), :]
            dst = self.got.at[part]
        else:
            src = dst = self.out.at[part, pl.ds(pl.multiple_of(self.core * self.half_rows, 16), self.half_rows), :]
        return pltpu.make_async_remote_copy(src_ref=src, dst_ref=dst, send_sem=self.pair_sem.at[0, which, part], recv_sem=self.pair_sem.at[1, which, part],
                                            device_id={'dap': 1 - self.core}, device_id_type=MESH)

    def ring_copy(self, part, leg, offset):
        axis = ORDERS[part][(0, 1, 2, 1, 0)[leg]]
        here = (self.dp // STRIDES[axis]) % RING
        peer = (here + offset) % RING
        if leg == 0:
            src = self.half.at[part, pl.ds(pl.multiple_of(peer * self.long_rows, 16), self.long_rows), :]
            dst = self.long_got.at[part, offset - 1]
        elif leg == 1 and self.scatter:
            src = self.long.at[part, pl.ds(pl.multiple_of(peer * self.short_rows, 16), self.short_rows), :]
            dst = self.mid.at[part, offset - 1]
        elif leg == 1:
            src = dst = self.mid.at[part, here]
        elif leg == 2:
            src = dst = self.last.at[part, here]
        elif leg == 3:
            src = dst = self.whole.at[part, pl.ds(pl.multiple_of(here * self.short_rows, 16), self.short_rows), :]
        else:
            src, dst = self.whole.at[part], self.out.at[part, self.own_rows(part), :]
        return pltpu.make_async_remote_copy(src_ref=src, dst_ref=dst, send_sem=self.sem.at[0, leg, part, offset - 1], recv_sem=self.sem.at[1, leg, part, offset - 1],
                                            device_id={'dp': self.dp + (peer - here) * STRIDES[axis]}, device_id_type=MESH)

    def own_rows(self, part):
        return pl.ds(pl.multiple_of(self.core * self.half_rows + self.coord(part, 0) * self.long_rows, 16), self.long_rows)

    def own_copy(self, part, which):
        if which == 0:
            src, dst = self.src.at[part, pl.ds(pl.multiple_of(self.core * self.half_rows, 16), self.half_rows), :], self.half.at[part]
        else:
            src, dst = self.whole.at[part], self.out.at[part, self.own_rows(part), :]
        return pltpu.make_async_copy(src, dst, self.own_sem.at[which, part])

    def send(self, part, leg):
        for offset in range(1, RING):
            self.ring_copy(part, leg, offset).start()

    def arrive(self, part, leg):
        for offset in range(1, RING):
            self.ring_copy(part, leg, offset).wait_recv()

    def add(self, rows, put, gets):
        def step(i, carry):
            at = pl.multiple_of(i * self.block, 16)
            total = gets[0](at).astype(F32)
            for get in gets[1:]:
                total += get(at).astype(F32)
            put(at, total.astype(BF16))
            return carry

        lax.fori_loop(0, rows // self.block, step, 0)

    def reader(self, ref, *lead, base=0):
        return lambda at: ref[(*lead, pl.ds(pl.multiple_of(base + at, 16), self.block), slice(None))]

    def writer(self, ref, *lead, base=0):
        def put(at, values):
            ref[(*lead, pl.ds(pl.multiple_of(base + at, 16), self.block), slice(None))] = values
        return put

    def start(self):
        for part in range(3):
            self.pair_copy(part, 0).start()
            if self.scatter:
                self.own_copy(part, 0).start()

    def step(self, number):
        for part in range(3):
            self.part_step(number, part)

    def part_step(self, number, part):
        half, long, short = self.half_rows, self.long_rows, self.short_rows
        if number == 0:
            self.pair_copy(part, 0).wait_recv()
            if self.scatter:
                self.own_copy(part, 0).wait()
                mine = self.reader(self.half, part)
            else:
                mine = self.reader(self.src, part, base=self.core * half)
            self.add(half, self.writer(self.half, part), [mine, self.reader(self.got, part)])
            self.send(part, 0)
        elif number == 1:
            self.arrive(part, 0)
            gets = [self.reader(self.half, part, base=self.coord(part, 0) * long)] + [self.reader(self.long_got, part, i) for i in range(RING - 1)]
            put = self.writer(self.long, part) if self.scatter else self.writer(self.mid, part, self.coord(part, 1))
            self.add(long, put, gets)
            self.send(part, 1)
        elif number == 2:
            self.arrive(part, 1)
            if self.scatter:
                gets = [self.reader(self.long, part, base=self.coord(part, 1) * short)] + [self.reader(self.mid, part, i) for i in range(RING - 1)]
            else:
                gets = [self.reader(self.mid, part, i) for i in range(RING)]
            self.add(short, self.writer(self.last, part, self.coord(part, 2)), gets)
            self.send(part, 2)
        elif number == 3:
            self.arrive(part, 2)
            gets = [self.reader(self.last, part, i) for i in range(RING)]
            if self.scatter:
                self.add(short, self.writer(self.whole, part, base=self.coord(part, 1) * short), gets)
                self.send(part, 3)
            else:
                self.add(short, self.writer(self.whole, part), gets)
                self.own_copy(part, 1).start()
                self.send(part, 4)
        elif number == 4 and self.scatter:
            self.arrive(part, 3)
            self.own_copy(part, 1).start()
            self.send(part, 4)
        elif number == 5:
            self.arrive(part, 4)
            self.own_copy(part, 1).wait()
            self.pair_copy(part, 1).start()
        elif number == 6:
            self.pair_copy(part, 1).wait_recv()
            for which in range(2):
                self.pair_copy(part, which).wait_send()
            for leg in range(5):
                if leg != 3 or self.scatter:
                    for offset in range(1, RING):
                        self.ring_copy(part, leg, offset).wait_send()


NUM_STEPS = 7


def enter_barrier():
    barrier = pltpu.get_barrier_semaphore()
    dp = lax.axis_index('dp')
    pl.semaphore_signal(barrier, inc=1, device_id={'dap': 1 - lax.axis_index('dap')}, device_id_type=MESH)
    for stride in STRIDES:
        here = (dp // stride) % RING
        for offset in range(1, RING):
            pl.semaphore_signal(barrier, inc=1, device_id={'dp': dp + ((here + offset) % RING - here) * stride}, device_id_type=MESH)
    pl.semaphore_wait(barrier, 1 + 3 * (RING - 1))


VMEM_LIMIT = 60 * 1024 * 1024
BIG_VMEM = 67043328


def solution(mesh):
    pair_spec = P('dp', 'dap', None, None)
    single_spec = P('dp', 'dap', None)

    def body(pair_z, single_s, token_mask, dz_out, ds_out, w_pa, w_pb, w_po, w_bias, w_q, q_bias, w_kv, w_g, w_o, w_sa, w_sb, w_so):
        num_cplx, num_rows, num_tok, chans = pair_z.shape
        s_chans = single_s.shape[2]
        width = w_pa.shape[1]
        idx = lax.axis_index('dap')
        swap = [(0, 1), (1, 0)]
        other_s = lax.ppermute(single_s, 'dap', swap)
        w_bias_t = w_bias.T
        steps = num_rows // ROWS
        row_spec = pl.BlockSpec((1, ROWS, num_tok, chans), lambda c, r: (c, r, 0, 0))
        head_spec = pl.BlockSpec((1, HEADS * num_rows, num_tok), lambda c, r: (c, 0, 0))

        def whole(shape):
            return pl.BlockSpec(shape, lambda c, r: (0,) * len(shape))

        positions = num_cplx * num_rows * num_tok
        z_new, bias = pl.pallas_call(
            pair_forward_kernel,
            grid=(num_cplx, steps),
            in_specs=[row_spec, whole(w_pa.shape), whole(w_pb.shape), whole(w_po.shape), whole(w_bias_t.shape)],
            out_specs=[row_spec, head_spec],
            out_shape=[jax.ShapeDtypeStruct(pair_z.shape, BF16), jax.ShapeDtypeStruct((num_cplx, HEADS * num_rows, num_tok), F32)],
            compiler_params=pltpu.CompilerParams(dimension_semantics=('arbitrary', 'arbitrary'), vmem_limit_bytes=VMEM_LIMIT),
            cost_estimate=pl.CostEstimate(flops=positions * 3 * 2 * chans * width, bytes_accessed=positions * chans * 4, transcendentals=positions * width),
            name='pair_forward',
        )(pair_z, w_pa, w_pb, w_po, w_bias_t)

        tokens = num_cplx * num_rows
        pack, d_logits, send, grad_mid, grad_act = pl.pallas_call(
            single_kernel,
            in_specs=[pl.BlockSpec(memory_space=pltpu.SMEM)] + [pl.BlockSpec(memory_space=pltpu.VMEM)] * 13,
            out_specs=[pl.BlockSpec(memory_space=pltpu.VMEM)] * 5,
            out_shape=[
                jax.ShapeDtypeStruct((3, PACK_ROWS, LANES), BF16),
                jax.ShapeDtypeStruct((num_cplx, HEADS * num_rows, num_tok), F32),
                jax.ShapeDtypeStruct((tokens, s_chans), BF16),
                jax.ShapeDtypeStruct((tokens, s_chans), F32),
                jax.ShapeDtypeStruct((tokens, s_chans), F32),
            ],
            scratch_shapes=[pltpu.VMEM((2 * tokens, s_chans), BF16), pltpu.VMEM((2 * tokens, s_chans), F32)],
            compiler_params=pltpu.CompilerParams(vmem_limit_bytes=VMEM_LIMIT),
            cost_estimate=pl.CostEstimate(flops=10 ** 10, bytes_accessed=10 ** 7, transcendentals=10 ** 6),
            name='single_path',
        )(idx.reshape(1).astype(jnp.int32), single_s, other_s, token_mask, ds_out, bias, w_q, q_bias.reshape(1, s_chans), w_kv, w_g, w_o, w_sa, w_sb, w_so)

        recv = lax.ppermute(send, 'dap', swap)

        num_steps = num_cplx * steps
        last = num_steps - 1
        block = (1, ROWS, num_tok, chans)

        def at_row(row):
            return (row // steps, row % steps, 0, 0)

        dz_in, pack, pair_pack = pl.pallas_call(
            backward_kernel,
            grid=(2, num_steps),
            in_specs=[
                pl.BlockSpec(block, lambda p, r: at_row(r)),
                pl.BlockSpec(block, lambda p, r: at_row(r * (1 - p) + last * p)),
                pl.BlockSpec(block, lambda p, r: at_row(r * (1 - p) + last * p)),
                pl.BlockSpec((1, HEADS * num_rows, num_tok), lambda p, r: ((r * (1 - p) + last * p) // steps, 0, 0)),
                whole(w_pa.shape), whole(w_pb.shape), whole(w_po.shape), whole(w_bias_t.shape),
                pl.BlockSpec(memory_space=pl.ANY),
            ],
            out_specs=[pl.BlockSpec(block, lambda p, r: at_row(r * p)), pl.BlockSpec(memory_space=pl.ANY), pl.BlockSpec(memory_space=pl.ANY)],
            out_shape=[
                jax.ShapeDtypeStruct(pair_z.shape, BF16),
                jax.ShapeDtypeStruct(pack.shape, BF16),
                jax.ShapeDtypeStruct((3, PAIR_ROWS, LANES), BF16),
            ],
            scratch_shapes=[
                pltpu.VMEM((chans, width), F32), pltpu.VMEM((chans, width), F32), pltpu.VMEM((chans, width), F32), pltpu.VMEM((HEADS, chans), F32),
                pltpu.VMEM((3, PAIR_ROWS, LANES), BF16),
                pltpu.VMEM((num_steps, ROWS * num_tok, width), BF16), pltpu.VMEM((num_steps, ROWS * num_tok, width), BF16),
                pltpu.VMEM((num_steps, ROWS * num_tok, chans), BF16),
            ] + reduce_scratch(PACK_ROWS, True) + reduce_scratch(PAIR_ROWS, False),
            compiler_params=pltpu.CompilerParams(dimension_semantics=('arbitrary', 'arbitrary'), vmem_limit_bytes=BIG_VMEM, collective_id=0, has_side_effects=True),
            cost_estimate=pl.CostEstimate(flops=positions * 8 * 2 * chans * width, bytes_accessed=positions * chans * 8, transcendentals=positions * width),
            name='pair_backward',
        )(pair_z, z_new, dz_out, d_logits, w_pa, w_pb, w_po, w_bias_t, pack)

        grad_shapes = [w_pa.shape, w_pb.shape, w_po.shape, w_bias_t.shape, w_q.shape, (1, s_chans), w_kv.shape, w_g.shape, w_o.shape, w_sa.shape, w_sb.shape, w_so.shape]
        outs = pl.pallas_call(
            finish_kernel,
            in_specs=[pl.BlockSpec(memory_space=pltpu.VMEM)] * 6,
            out_specs=[pl.BlockSpec(memory_space=pltpu.VMEM)] * 13,
            out_shape=[jax.ShapeDtypeStruct((tokens, s_chans), BF16)] + [jax.ShapeDtypeStruct(shape, F32) for shape in grad_shapes],
            compiler_params=pltpu.CompilerParams(vmem_limit_bytes=VMEM_LIMIT),
            name='finish',
        )(single_s.reshape(tokens, s_chans), grad_mid, grad_act, recv, pack, pair_pack)
        ds_in = outs[0].reshape(single_s.shape)
        grads = list(outs[1:])
        grads[3] = grads[3].T
        grads[5] = grads[5].reshape(s_chans)
        return (dz_in, ds_in, *grads)

    in_specs = (pair_spec, single_spec, P('dp', None), pair_spec, single_spec) + (P(),) * 12
    out_specs = (pair_spec, single_spec) + (P(),) * 12
    return jax.shard_map(body, mesh=mesh, in_specs=in_specs, out_specs=out_specs, check_vma=False)
```
